32 devices in a mesh: gx: 4 (over y, x), gy: 8 (over z, core).
Axes of the slice: x: 2, y: 2, z: 4, core: 2. Of those that a mesh axis runs over, the one named last changes fastest.
Arguments:
- primal: float32 [4, 27, 16384], P(None, None, ('gx', 'gy')), may hold values from -6 to 6
- adjoint: float32 [4, 27, 16384], P(None, None, ('gx', 'gy')), may hold values from -6 to 6
- source: float32 [4, 27, 16384], P(None, None, ('gx', 'gy')), may hold values from -6 to 6
- coefficient: float32 [16384], P(('gx', 'gy')), may hold values from 0.3 to 3
- levels: int32 [16384], P(('gx', 'gy')), may hold values from 0 to 3
- recon: float32 [7, 125, 27], replicated, may hold values from -0.4375 to 0.4375
- stiffness: float32 [125, 27], replicated, may hold values from -1.25 to 1.25
- interp: float32 [125, 27], replicated, may hold values from -1.25 to 1.25
- flux: float32 [6, 25, 27], replicated, may hold values from -1.25 to 1.25
- face_eval: float32 [6, 25, 125], replicated, may hold values from -0.5 to 0.5
- child_interp: float32 [4, 25, 25], replicated, may hold values from -1.25 to 1.25
- ghost_send: int32 [32, 8, 32], P(('gx', 'gy')), may hold values from -1 to 511, as said below
- edge_send: int32 [32, 2, 16], P(('gx', 'gy')), may hold values from -1 to 511, as said below
- neighbor_slot: int32 [6, 16384], P(None, ('gx', 'gy')), may hold values from -1 to 799, as said below
- neighbor_child: int32 [6, 16384], P(None, ('gx', 'gy')), may hold values from 0 to 4, as said below
- hang_send: int32 [2, 32, 8, 8], P(None, ('gx', 'gy')), may hold values from -1 to 511, as said below
- hang_recv: int32 [3, 32, 8, 8], P(None, ('gx', 'gy')), may hold values from -1 to 511, as said below
Outputs:
- cell_indicator: float32 [4, 16384], P(None, ('gx', 'gy'))
- face_indicator: float32 [4, 16384], P(None, ('gx', 'gy'))
The draws below stay inside these ranges and needn't reach their ends.
Inputs may be any that keep to these rules, and one draw needn't show every extreme that they name: `ghost_send`: the gy index of a device numbers a block of a cube of blocks with side S, the cube root of 8: index = G(c0) + S * G(c1) + S * S * G(c2) for block coordinates c0, c1, c2, where G(p) = p xor (p // 2) is the Gray code, so face-adjacent blocks differ in one bit of the index. Row [r, p] lists the local cells that device r sends to the device with its gx index and gy index p, live ids first, then -1. Only the up to six blocks face-adjacent to r's block get live ids, between 16 and 32 of them, and exactly 32 go to the neighbour one step up along coordinate 0 wherever it exists. `edge_send`: row [r, 0] lists the local cells sent to the device one gx index lower with the same gy index, row [r, 1] those sent to the one higher, live ids first, then -1; where that device exists there are 8 to 16 live ids, and exactly 16 towards the lower one; otherwise the row is all -1. `neighbor_slot`: every slot that is not -1 points at a live entry: a cell of the device itself, a live entry of a gy peer's ghost_send row for this device, or a live entry of a gx neighbour's edge_send row towards this device. `neighbor_child`: 4 means a neighbour of the same level. `hang_send`: [0, r, p, t] is a local cell of device r and [1, r, p, t] one of its faces, both -1 after the live slots; live slots go only to face-adjacent gy peers (as for ghost_send), at most 8 to one peer, and the device with gy index 0 sends exactly 8 to each of its face-adjacent peers. `hang_recv`: [:, q, p, t] describes what device q receives in slot t from the device with its gx index and gy index p: a local coarse cell, its face (the opposite of the sender's fine face) and a child position 0 to 3; all three are -1 exactly where the sender's slot is empty.
All inputs are finite; a program needn't handle non-finite values.
Results may differ from the reference program's by a relative error of at most 0.0003.
Values sent between devices are 32-bit elements; how exact they have to be, the bound alone decides.
A program may use at most 128 MiB of HBM per device.

```python
import math
import jax
import jax.numpy as jnp
from jax import lax

F = 4
DOFS = 27
QUADS = 125
FACEPTS = 25
CELL_DEV = 512
GSLOT = 32
XSLOT = 16
HSLOT = 8
CELLS = 16384
N_GY = 8
DEVICES = 32


def gray_encode(position):
    return jnp.bitwise_xor(position, position >> 1)


def gray_decode(code, side_log):
    position = code
    for shift_by in range(1, max(side_log, 1)):
        position = jnp.bitwise_xor(position, code >> shift_by)
    return position


def block_table():
    side_log = (N_GY.bit_length() - 1) // 3
    length = 1 << side_log
    own_rows = jnp.arange(N_GY, dtype=jnp.int32)
    coords = [gray_decode(own_rows >> side_log * axis_dim & length - 1, side_log) for axis_dim in range(3)]
    columns = []
    for axis_dim in range(3):
        for direction in (1, -1):
            moved = [coords[other] + (direction if other == axis_dim else 0) for other in range(3)]
            inside = (moved[axis_dim] >= 0) & (moved[axis_dim] < length)
            block_index = jnp.zeros((N_GY,), jnp.int32)
            for other in range(3):
                block_index = block_index + (gray_encode(moved[other] & length - 1) << side_log * other)
            columns.append(jnp.where(inside, block_index, -1))
    return jnp.stack(columns, 1)


def mesh_layout(key):
    segments = DEVICES // N_GY
    table = block_table()
    device = jnp.arange(DEVICES, dtype=jnp.int32)
    own_row = device % N_GY
    segment = device // N_GY
    peer_rows = jnp.arange(N_GY, dtype=jnp.int32)
    row_table = table[own_row]
    near = jnp.any(row_table[:, :, None] == peer_rows[None, None, :], axis=1)
    full = row_table[:, 0:1] == peer_rows[None, :]
    count = jax.random.randint(jax.random.fold_in(key, 11), (DEVICES, N_GY), GSLOT // 2, GSLOT + 1)
    count = jnp.where(full, GSLOT, count)
    count = jnp.where(near, count, 0)
    ghost_ids = jax.random.randint(jax.random.fold_in(key, 12), (DEVICES, N_GY, GSLOT), 0, CELL_DEV)
    ghost = jnp.where(jnp.arange(GSLOT)[None, None, :] < count[:, :, None], ghost_ids, -1)
    has_side = jnp.stack([segment > 0, segment < segments - 1], 1)
    edge_count = jax.random.randint(jax.random.fold_in(key, 13), (DEVICES, 2), XSLOT // 2, XSLOT + 1)
    edge_count = jnp.where(jnp.arange(2)[None, :] == 0, XSLOT, edge_count)
    edge_count = jnp.where(has_side, edge_count, 0)
    edge_ids = jax.random.randint(jax.random.fold_in(key, 14), (DEVICES, 2, XSLOT), 0, CELL_DEV)
    edge = jnp.where(jnp.arange(XSLOT)[None, None, :] < edge_count[:, :, None], edge_ids, -1)
    shape = (DEVICES, 6, CELL_DEV)
    kind_draw = jax.random.randint(jax.random.fold_in(key, 15), shape, 0, 20)
    local_cell = jax.random.randint(jax.random.fold_in(key, 16), shape, 0, CELL_DEV)
    direction = jax.random.randint(jax.random.fold_in(key, 17), shape, 0, 6)
    row_wide = jnp.broadcast_to(own_row[:, None, None], shape)
    first_peer = table[row_wide, direction]
    other_peer = table[row_wide, jnp.bitwise_xor(direction, 1)]
    source_row = jnp.where(first_peer >= 0, first_peer, other_peer)
    sender = segment[:, None, None] * N_GY + source_row
    live_count = jnp.maximum(count[sender, row_wide], 1)
    draw_bits = jax.random.randint(jax.random.fold_in(key, 18), shape, 0, 1 << 20)
    via_segment = CELL_DEV + source_row * GSLOT + draw_bits % live_count
    side_draw = jax.random.randint(jax.random.fold_in(key, 19), shape, 0, 2)
    low_ok = (segment > 0)[:, None, None]
    high_ok = (segment < segments - 1)[:, None, None]
    side_pick = jnp.where(side_draw == 0, jnp.where(low_ok, 0, 1), jnp.where(high_ok, 1, 0))
    side_ok = jnp.where(side_pick == 0, low_ok, high_ok)
    edge_sender = jnp.clip(device[:, None, None] + (2 * side_pick - 1) * N_GY, 0, DEVICES - 1)
    edge_live = jnp.maximum(edge_count[edge_sender, 1 - side_pick], 1)
    via_edges = CELL_DEV + N_GY * GSLOT + side_pick * XSLOT + draw_bits % edge_live
    chosen = jnp.where(kind_draw < 10, local_cell, jnp.where(kind_draw < 17, via_segment, jnp.where((kind_draw < 19) & side_ok, via_edges, -1)))
    neighbours = jnp.transpose(chosen, (1, 0, 2)).reshape(6, DEVICES * CELL_DEV)
    heavy = (jax.random.randint(jax.random.fold_in(key, 20), (DEVICES,), 0, 4) == 0) | (own_row == 0)
    light = jax.random.randint(jax.random.fold_in(key, 21), (DEVICES, N_GY), 0, HSLOT // 2 + 1)
    hang_count = jnp.where(heavy[:, None], HSLOT, light)
    hang_count = jnp.where(near, hang_count, 0)
    hang_live = jnp.arange(HSLOT)[None, None, :] < hang_count[:, :, None]
    hang_shape = (DEVICES, N_GY, HSLOT)
    fine_cell = jax.random.randint(jax.random.fold_in(key, 22), hang_shape, 0, CELL_DEV)
    fine_face = jax.random.randint(jax.random.fold_in(key, 23), hang_shape, 0, 6)
    coarse_cell = jax.random.randint(jax.random.fold_in(key, 24), hang_shape, 0, CELL_DEV)
    child_pos = jax.random.randint(jax.random.fold_in(key, 25), hang_shape, 0, 4)

    def turned(values):
        masked = jnp.where(hang_live, values, -1)
        return masked.reshape(segments, N_GY, N_GY, HSLOT).transpose(0, 2, 1, 3).reshape(DEVICES, N_GY, HSLOT)
    sent = jnp.stack([jnp.where(hang_live, fine_cell, -1), jnp.where(hang_live, fine_face, -1)])
    received = jnp.stack([turned(coarse_cell), turned(jnp.bitwise_xor(fine_face, 1)), turned(child_pos)])
    return (ghost, edge, neighbours, sent, received)


def draw_ghost_send(key, part):
    return mesh_layout(key)[0].astype(jnp.int32)


def draw_edge_send(key, part):
    return mesh_layout(key)[1].astype(jnp.int32)


def draw_neighbor_slot(key, part):
    return mesh_layout(key)[2].astype(jnp.int32)


def draw_hang_send(key, part):
    return mesh_layout(key)[3].astype(jnp.int32)


def draw_hang_recv(key, part):
    return mesh_layout(key)[4].astype(jnp.int32)


def draw_neighbor_child(key, part):
    child_draw = jax.random.randint(jax.random.fold_in(key, 31), (6, CELLS), 0, 20)
    return jnp.where(child_draw < 16, 4, child_draw - 16).astype(jnp.int32)


def touch_ends(entries, stream_key, least, top_value):
    spot = [jax.random.randint(jax.random.fold_in(stream_key, axis), (), 0, length) for axis, length in enumerate(entries.shape)]
    longest = entries.shape.index(max(entries.shape))
    beside = spot[:longest] + [(spot[longest] + 1) % entries.shape[longest]] + spot[longest + 1:]
    return entries.at[tuple(spot)].set(least).at[tuple(beside)].set(top_value)


def block_levels(key, dims, shards, smallest, high):
    def one(dim, parts):
        heights = jax.random.uniform(jax.random.fold_in(jax.random.fold_in(key, 6), dim), (parts,), jnp.float32, smallest / len(shards), high / len(shards))
        return jnp.repeat(jnp.exp(heights), dims[dim] // parts).reshape((-1,) + (1,) * (len(dims) - dim - 1))

    gain = one(*shards[0])
    for cut in shards[1:]:
        gain = gain * one(*cut)
    return gain


def noise(own_key, dims, spread, limit, split=(), kind=jnp.bfloat16):
    values = spread * jax.random.normal(own_key, dims, jnp.float32)
    if split:
        values = values * block_levels(own_key, dims, split, -0.22, 0.18)
    return jnp.clip(values, -limit, limit).astype(kind)


def setup_inputs(seed: int = 0) -> dict:
    arg_keys = jax.random.split(jax.random.key(seed), 18)
    primal = noise(arg_keys[0], (F, DOFS, CELLS), 1.0, 6.0, ((2, 32),), jnp.float32)
    adjoint = noise(arg_keys[1], (F, DOFS, CELLS), 1.0, 6.0, ((2, 32),), jnp.float32)
    source = noise(arg_keys[2], (F, DOFS, CELLS), 1.0, 6.0, ((2, 32),), jnp.float32)
    coefficient = jnp.clip(jnp.exp(math.log(3.0) - 2.3025851 * jax.random.uniform(arg_keys[3], (CELLS,), jnp.float32) ** block_levels(arg_keys[3], (CELLS,), ((0, 32),), -0.2, 0.2)), 0.3, 3.0)
    levels = touch_ends(jax.random.randint(arg_keys[4], (CELLS,), 0, 4), jax.random.fold_in(arg_keys[4], 1), 0, 3).astype(jnp.int32)
    recon = noise(arg_keys[5], (7, QUADS, DOFS), (7 * DOFS) ** -0.5, 0.4375, (), jnp.float32)
    stiffness = noise(arg_keys[6], (QUADS, DOFS), DOFS ** -0.5, 1.25, (), jnp.float32)
    interp = noise(arg_keys[7], (QUADS, DOFS), DOFS ** -0.5, 1.25, (), jnp.float32)
    flux = noise(arg_keys[8], (6, FACEPTS, DOFS), DOFS ** -0.5, 1.25, (), jnp.float32)
    face_eval = noise(arg_keys[9], (6, FACEPTS, QUADS), QUADS ** -0.5, 0.5, (), jnp.float32)
    child_interp = noise(arg_keys[10], (4, FACEPTS, FACEPTS), FACEPTS ** -0.5, 1.25, (), jnp.float32)
    ghost_send = draw_ghost_send(jax.random.fold_in(arg_keys[17], 71), 0)
    edge_send = draw_edge_send(jax.random.fold_in(arg_keys[17], 71), 0)
    neighbor_slot = draw_neighbor_slot(jax.random.fold_in(arg_keys[17], 71), 0)
    neighbor_child = draw_neighbor_child(jax.random.fold_in(arg_keys[17], 71), 0)
    hang_send = draw_hang_send(jax.random.fold_in(arg_keys[17], 71), 0)
    hang_recv = draw_hang_recv(jax.random.fold_in(arg_keys[17], 71), 0)
    return dict(primal=primal, adjoint=adjoint, source=source, coefficient=coefficient, levels=levels, recon=recon, stiffness=stiffness, interp=interp, flux=flux, face_eval=face_eval, child_interp=child_interp, ghost_send=ghost_send, edge_send=edge_send, neighbor_slot=neighbor_slot, neighbor_child=neighbor_child, hang_send=hang_send, hang_recv=hang_recv)


PRECISE = lax.Precision.HIGHEST
OPPOSITE = (1, 0, 3, 2, 5, 4)

def collect(blocks, cell_ids):
    safe_cells = jnp.maximum(cell_ids, 0)
    taken = jnp.take(blocks, safe_cells.reshape(-1), axis=2)
    taken = taken.reshape(blocks.shape[:2] + cell_ids.shape)
    return jnp.where(cell_ids >= 0, taken, 0.0)

def face_traces(flux, primal, cell_ids, face_ids):
    fine_u = collect(primal, cell_ids)
    flat_u = fine_u.reshape(fine_u.shape[0], fine_u.shape[1], -1)
    flat_faces = face_ids.reshape(-1)
    chosen = jnp.zeros((flat_u.shape[0], flux.shape[1], flat_u.shape[2]), jnp.float32)
    for face_idx in range(6):
        term = jnp.einsum('pj,kjs->kps', flux[face_idx], flat_u, precision=PRECISE)
        chosen = chosen + jnp.where(flat_faces == face_idx, term, 0.0)
    return chosen.reshape(chosen.shape[:2] + cell_ids.shape)

def take_back(face_total, traces_in, recv_maps, face_weight, child_interp):
    flat_trace = traces_in.reshape(traces_in.shape[0], traces_in.shape[1], -1)
    coarse = recv_maps[0].reshape(-1)
    coarse_face = recv_maps[1].reshape(-1)
    child_pos = recv_maps[2].reshape(-1)
    lifted = jnp.zeros_like(flat_trace)
    for position in range(4):
        term = jnp.einsum('qp,kqs->kps', child_interp[position], flat_trace, precision=PRECISE)
        lifted = lifted + jnp.where(child_pos == position, term, 0.0)
    target = jnp.maximum(coarse, 0)
    chosen = jnp.zeros_like(flat_trace)
    for face_idx in range(6):
        chosen = chosen + jnp.where(coarse_face == face_idx, jnp.take(face_weight[face_idx], target, axis=2), 0.0)
    contrib = jnp.where(coarse >= 0, lax.optimization_barrier(jnp.sum(lifted * chosen, axis=1)), 0.0)
    return face_total.at[:, target].add(contrib)

def local_terms(primal, adjoint, source, coefficient, recon, stiffness, interp, flux, face_eval, child_interp, primal_near, adjoint_near, buffer_slots, neighbor_child):
    is_live = buffer_slots >= 0
    safe_cells = jnp.maximum(buffer_slots, 0)
    weight = jnp.einsum('qj,kjc->kqc', recon[0], adjoint, precision=PRECISE)
    for face_idx in range(6):
        near_z = jnp.where(is_live[face_idx], jnp.take(adjoint_near, safe_cells[face_idx], axis=2), 0.0)
        weight = weight + jnp.einsum('qj,kjc->kqc', recon[face_idx + 1], near_z, precision=PRECISE)
    residual_q = jnp.einsum('qj,kjc->kqc', interp, source, precision=PRECISE) - coefficient * jnp.einsum('qj,kjc->kqc', stiffness, primal, precision=PRECISE)
    cell_part = lax.optimization_barrier(jnp.sum(residual_q * weight, axis=1))
    face_weight = jnp.einsum('fpq,kqc->fkpc', face_eval, weight, precision=PRECISE)
    face_total = jnp.zeros(cell_part.shape, jnp.float32)
    for face_idx in range(6):
        near_u = jnp.where(is_live[face_idx], jnp.take(primal_near, safe_cells[face_idx], axis=2), 0.0)
        outer_trace = jnp.einsum('pj,kjc->kpc', flux[OPPOSITE[face_idx]], near_u, precision=PRECISE)
        child_here = neighbor_child[face_idx]
        mapped = jnp.where(child_here == 4, outer_trace, 0.0)
        for position in range(4):
            term = jnp.einsum('pq,kqc->kpc', child_interp[position], outer_trace, precision=PRECISE)
            mapped = mapped + jnp.where(child_here == position, term, 0.0)
        inner_trace = jnp.einsum('pj,kjc->kpc', flux[face_idx], primal, precision=PRECISE)
        face_total = face_total + lax.optimization_barrier(jnp.sum((inner_trace + mapped) * face_weight[face_idx], axis=1))
    return (cell_part, face_total, face_weight)

def finish(cell_part, face_total, levels, quad_count, point_count):
    cell_size = jnp.exp2(-levels.astype(jnp.float32))
    return (cell_size * cell_part / math.sqrt(quad_count), cell_size * face_total / math.sqrt(6 * point_count))

def reference(primal, adjoint, source, coefficient, levels, recon, stiffness, interp, flux, face_eval, child_interp, ghost_send, edge_send, neighbor_slot, neighbor_child, hang_send, hang_recv):
    fields = primal.shape[0]

    def device(device_id):
        own_row = device_id % N_GY
        segment = device_id // N_GY
        first_cell = (device_id * CELL_DEV).astype(jnp.int32)
        own_u = lax.dynamic_slice_in_dim(primal, first_cell, CELL_DEV, 2)
        own_z = lax.dynamic_slice_in_dim(adjoint, first_cell, CELL_DEV, 2)
        own_src = lax.dynamic_slice_in_dim(source, first_cell, CELL_DEV, 2)
        coeff_cells = lax.dynamic_slice_in_dim(coefficient, first_cell, CELL_DEV, 0)
        level_cells = lax.dynamic_slice_in_dim(levels, first_cell, CELL_DEV, 0)
        slot_rows = lax.dynamic_slice_in_dim(neighbor_slot, first_cell, CELL_DEV, 1)
        child_rows = lax.dynamic_slice_in_dim(neighbor_child, first_cell, CELL_DEV, 1)
        shifted = slot_rows - CELL_DEV
        source_peer = jnp.clip(shifted // GSLOT, 0, N_GY - 1)
        ghost_pos = jnp.clip(shifted - source_peer * GSLOT, 0, GSLOT - 1)
        sender = segment * N_GY + source_peer
        via_segment = sender * CELL_DEV + ghost_send[sender, own_row, ghost_pos]
        edge_rel = shifted - N_GY * GSLOT
        side_pick = jnp.clip(edge_rel // XSLOT, 0, 1)
        edge_pos = jnp.clip(edge_rel - side_pick * XSLOT, 0, XSLOT - 1)
        edge_sender = jnp.clip(device_id + (2 * side_pick - 1) * N_GY, 0, DEVICES - 1)
        via_edges = edge_sender * CELL_DEV + edge_send[edge_sender, 1 - side_pick, edge_pos]
        global_ids = jnp.where(slot_rows < 0, -1, jnp.where(slot_rows < CELL_DEV, first_cell + slot_rows, jnp.where(shifted < N_GY * GSLOT, via_segment, via_edges)))
        global_ids = global_ids.astype(jnp.int32)
        cell_part, face_total, face_weight = local_terms(own_u, own_z, own_src, coeff_cells, recon, stiffness, interp, flux, face_eval, child_interp, primal, adjoint, global_ids, child_rows)
        senders = segment * N_GY + jnp.arange(N_GY, dtype=jnp.int32)
        fine_cell = hang_send[0][senders, own_row]
        fine_face = hang_send[1][senders, own_row]
        fine_ids = jnp.where(fine_cell >= 0, senders[:, None] * CELL_DEV + fine_cell, -1).astype(jnp.int32)
        traces_in = face_traces(flux, primal, fine_ids, fine_face)
        recv_maps = hang_recv[:, device_id]
        face_total = take_back(face_total, traces_in, recv_maps, face_weight, child_interp)
        return finish(cell_part, face_total, level_cells, recon.shape[1], flux.shape[1])
    cell_parts, face_parts = lax.map(device, jnp.arange(DEVICES, dtype=jnp.int32))
    cell_indicator = jnp.transpose(cell_parts, (1, 0, 2)).reshape(fields, DEVICES * CELL_DEV)
    face_indicator = jnp.transpose(face_parts, (1, 0, 2)).reshape(fields, DEVICES * CELL_DEV)
    return (cell_indicator, face_indicator)
```

```python
import functools
import math

import jax
import jax.numpy as jnp
from jax import lax
from jax.experimental import pallas as pl
from jax.experimental.pallas import tpu as pltpu
from jax.sharding import PartitionSpec as P

LANES = 128
F32 = jnp.float32
BF16 = jnp.bfloat16
MESH = pl.DeviceIdType.MESH


def round_up(value, unit):
    return -(-value // unit) * unit


def split(x):
    hi = x.astype(BF16)
    lo = (x - hi.astype(F32)).astype(BF16)
    return hi, lo


def mm(a, b):
    return jnp.dot(a, b, preferred_element_type=F32)


def dot3(a_both, b_hi, b_lo):
    rows = a_both.shape[0] // 2
    first = mm(a_both, b_hi)
    return first[:rows] + first[rows:] + mm(a_both[:rows], b_lo)


def fill_flat(flat, refs, width):
    for at, ref in enumerate(refs):
        dofs, fields, cells = ref.shape
        used = dofs * fields
        for i in range(cells // LANES):
            for j in range(dofs):
                row = at * width + j * fields
                flat[i, row : row + fields, :] = ref[j, :, i * LANES : (i + 1) * LANES]
            flat[i, at * width + used : (at + 1) * width, :] = jnp.zeros((width - used, LANES), F32)


def lane_gather(blocks, lane, block_id):
    total = jnp.zeros(blocks[0].shape, F32)
    for i, block in enumerate(blocks):
        got = jnp.take_along_axis(block, lane, axis=1)
        total = jnp.where(block_id == i, got, total)
    return total


def exchange_kernel(
    dims,
    primal_ref,
    adjoint_ref,
    ghost_ref,
    edge_ref,
    hang_ref,
    from_gy,
    from_gx,
    to_gy,
    to_gx,
    ids,
    packed,
    flat,
    send_gy,
    recv_gy,
    send_gx,
    recv_gx,
):
    n_gx, n_gy, bits, ghosts, edges, hangs, fields, rows = dims
    gx = lax.axis_index("gx")
    gy = lax.axis_index("gy")
    dofs, _, cells = primal_ref.shape
    width = fields * rows
    partners = [jnp.bitwise_xor(gy, 1 << b) for b in range(bits)]

    barrier = pltpu.get_barrier_semaphore()
    for partner in partners:
        pl.semaphore_signal(barrier, inc=1, device_id=(gx, partner), device_id_type=MESH)

    @pl.when(gx > 0)
    def _():
        pl.semaphore_signal(barrier, inc=1, device_id=(gx - 1, gy), device_id_type=MESH)

    @pl.when(gx < n_gx - 1)
    def _():
        pl.semaphore_signal(barrier, inc=1, device_id=(gx + 1, gy), device_id_type=MESH)

    main = bits * ghosts + 2 * edges
    main_pad = round_up(main, LANES)
    hang_pad = round_up(bits * hangs, LANES)
    ids[...] = jnp.zeros_like(ids)
    for b, partner in enumerate(partners):
        ids[0:1, b * ghosts : (b + 1) * ghosts] = ghost_ref[0, pl.ds(partner, 1), :]
        at = main_pad + b * hangs
        ids[0:1, at : at + hangs] = hang_ref[0, 0, pl.ds(partner, 1), :]
    for side in range(2):
        at = bits * ghosts + side * edges
        ids[0:1, at : at + edges] = edge_ref[0, side : side + 1, :]
    fill_flat(flat, (primal_ref, adjoint_ref), width)
    chosen = jnp.maximum(ids[0:1, :], 0)
    for at in range(0, main_pad + hang_pad, LANES):
        part = jnp.broadcast_to(chosen[:, at : at + LANES], (rows, LANES))
        lane = jnp.bitwise_and(part, LANES - 1)
        block_id = jnp.right_shift(part, 7)
        count = 2 * fields if at < main_pad else fields
        for group in range(count):
            blocks = [flat[i, group * rows : (group + 1) * rows, :] for i in range(cells // LANES)]
            packed[group * rows : (group + 1) * rows, :] = lane_gather(blocks, lane, block_id)
        if at < main_pad:
            turned = packed[...].T
            for first in range(at, min(at + LANES, main), edges):
                chunk = turned[first - at : first - at + edges]
                if first < bits * ghosts:
                    inner = first % ghosts
                    to_gy[first // ghosts, inner : inner + edges, :] = chunk
                else:
                    to_gx[(first - bits * ghosts) // edges] = chunk
        else:
            turned = packed[0:width, :].T
            for b in range(bits):
                at_slot = b * hangs - (at - main_pad)
                if 0 <= at_slot < LANES:
                    to_gy[b, ghosts : ghosts + hangs, 0:width] = turned[at_slot : at_slot + hangs]
                    to_gy[b, ghosts : ghosts + hangs, width:] = jnp.zeros(
                        (hangs, to_gy.shape[2] - width), F32
                    )

    def low_copy():
        return pltpu.make_async_remote_copy(
            src_ref=to_gx.at[0],
            dst_ref=from_gx.at[1],
            send_sem=send_gx.at[0],
            recv_sem=recv_gx.at[1],
            device_id=(gx - 1, gy),
            device_id_type=MESH,
        )

    def high_copy():
        return pltpu.make_async_remote_copy(
            src_ref=to_gx.at[1],
            dst_ref=from_gx.at[0],
            send_sem=send_gx.at[1],
            recv_sem=recv_gx.at[0],
            device_id=(gx + 1, gy),
            device_id_type=MESH,
        )

    @pl.when((gx > 0) & (gx < n_gx - 1))
    def _():
        pl.semaphore_wait(barrier, bits + 2)

    @pl.when((gx == 0) | (gx == n_gx - 1))
    def _():
        pl.semaphore_wait(barrier, bits + (1 if n_gx > 1 else 0))

    copies = []
    for b in reversed(range(bits)):
        copy = pltpu.make_async_remote_copy(
            src_ref=to_gy.at[b],
            dst_ref=from_gy.at[b],
            send_sem=send_gy.at[b],
            recv_sem=recv_gy.at[b],
            device_id=(gx, partners[b]),
            device_id_type=MESH,
        )
        copy.start()
        copies.append(copy)

    @pl.when(gx > 0)
    def _():
        low_copy().start()

    @pl.when(gx == 0)
    def _():
        from_gx[0] = jnp.zeros(from_gx.shape[1:], F32)

    @pl.when(gx < n_gx - 1)
    def _():
        high_copy().start()

    @pl.when(gx == n_gx - 1)
    def _():
        from_gx[1] = jnp.zeros(from_gx.shape[1:], F32)

    for copy in copies:
        copy.wait()

    @pl.when(gx > 0)
    def _():
        low_copy().wait_send()
        high_copy().wait_recv()

    @pl.when(gx < n_gx - 1)
    def _():
        high_copy().wait_send()
        low_copy().wait_recv()


def compute_kernel(
    dims,
    primal_ref,
    adjoint_ref,
    source_ref,
    coef_ref,
    levels_ref,
    recon_ref,
    stiffness_ref,
    interp_ref,
    flux_ref,
    face_eval_ref,
    child_interp_ref,
    slot_ref,
    child_ref,
    hang_ref,
    from_gy,
    from_gx,
    cell_ref,
    face_ref,
    op_recon,
    op_res,
    op_face,
    op_child,
    child_flat,
    op_flux,
    op_map,
    maps,
    z_hi,
    z_lo,
    u_hi,
    u_lo,
    sources,
    flat,
    source_flat,
    hang_flat,
):
    n_gx, n_gy, bits, ghosts, edges, hangs, fields, rows = dims
    gy = lax.axis_index("gy")
    dofs, _, cells = primal_ref.shape
    quads = recon_ref.shape[2]
    own_blocks = cells // LANES
    width = fields * rows
    points = flux_ref.shape[1]
    remote = bits * ghosts + 2 * edges
    remote_pad = round_up(remote, LANES)
    hang_count = bits * hangs
    hang_pad = round_up(hang_count, LANES)
    hang_rows = round_up(hang_count, 16)
    children = 4

    op_recon[...] = jnp.zeros_like(op_recon)
    op_res[...] = jnp.zeros_like(op_res)
    op_face[...] = jnp.zeros_like(op_face)
    child_flat[...] = jnp.zeros_like(child_flat)
    op_flux[...] = jnp.zeros_like(op_flux)
    for j in range(dofs):
        op_recon[8 * j : 8 * j + 7, 0:quads] = recon_ref[j]
    op_res[0:dofs, 0:quads] = interp_ref[...]
    op_res[rows : rows + dofs, 0:quads] = stiffness_ref[...]
    for f in range(6):
        op_face[f * rows : f * rows + points, 0:quads] = face_eval_ref[f]
        op_flux[0:points, f * rows : f * rows + dofs] = flux_ref[f]
    for p in range(points):
        child_flat[children * p : children * (p + 1), 0:points] = child_interp_ref[p]
    for h in range(children):
        op_child[h * rows : (h + 1) * rows, :] = child_flat[pl.ds(h, rows, stride=children), :]
    flux_all = op_flux[...]
    flux_hi, flux_lo = split(flux_all)
    child_both = jnp.concatenate(split(op_child[...]), 0)
    mapped_ops = dot3(child_both[:, 0:rows], flux_hi, flux_lo)
    for f in range(6):
        opp = f ^ 1
        for h in range(children):
            op_map[f, :, h * rows : (h + 1) * rows] = mapped_ops[
                h * rows : (h + 1) * rows, opp * rows : (opp + 1) * rows
            ]
        op_map[f, :, 4 * rows : 5 * rows] = flux_all[:, opp * rows : (opp + 1) * rows]
        op_map[f, :, 5 * rows : 6 * rows] = flux_all[:, f * rows : (f + 1) * rows]
    recon_turned = [op_recon[pl.ds(f, rows, stride=8), :] for f in range(8)]
    recon_both = jnp.concatenate(split(jnp.concatenate(recon_turned, 0).T), 0)
    res_both = jnp.concatenate(split(op_res[...].T), 0)
    face_both = jnp.concatenate(split(op_face[...]), 0)
    flux_both = jnp.concatenate([flux_hi, flux_lo], 0)[:, 0 : 6 * rows]
    back_both = jnp.concatenate(split(op_child[...].T[0:rows]), 0)
    map_both = [jnp.concatenate(split(op_map[f]), 0) for f in range(6)]

    maps[...] = jnp.full(maps.shape, -1, jnp.int32)
    for b in range(bits):
        partner = jnp.bitwise_xor(gy, 1 << b)
        for i in range(3):
            maps[i : i + 1, b * hangs : (b + 1) * hangs] = hang_ref[i, 0, pl.ds(partner, 1), :]
    lane_face = maps[1:2, :]
    lane_child = maps[2:3, :]
    live = maps[0:1, :] >= 0
    place = jnp.where(live, maps[0:1, :] + lane_face * cells, -1).astype(F32)
    place_rows = jnp.broadcast_to(place, (LANES, hang_pad)).T[0:hang_rows, 0:1]

    fill_flat(flat, (primal_ref, adjoint_ref), width)
    fill_flat(source_flat, (source_ref,), width)
    parts = [from_gy[b, 0:ghosts, :] for b in range(bits)] + [from_gx[0], from_gx[1]]
    if remote_pad > remote:
        parts.append(jnp.zeros((remote_pad - remote, parts[0].shape[1]), F32))
    arrived = jnp.concatenate(parts, 0).T
    for i in range(remote_pad // LANES):
        flat[own_blocks + i] = arrived[:, i * LANES : (i + 1) * LANES]
    n_blocks = own_blocks + remote_pad // LANES
    for i in range(n_blocks):
        for group in range(2 * fields):
            first = group // fields * width + group % fields
            sources[i, group * rows : (group + 1) * rows, :] = flat[
                i, pl.ds(first, rows, stride=fields), :
            ]
    parts = [from_gy[b, ghosts : ghosts + hangs, 0:width] for b in range(bits)]
    parts.append(jnp.zeros((hang_pad - hang_count, width), F32))
    hang_flat[...] = jnp.concatenate(parts, 0).T

    slot = slot_ref[...]
    shifted = slot - cells
    log_ghosts = ghosts.bit_length() - 1
    peer = jnp.right_shift(shifted, log_ghosts)
    within = jnp.bitwise_and(shifted, ghosts - 1)
    differing = jnp.bitwise_xor(peer, gy)
    packed = jnp.zeros_like(slot)
    for b in range(1, bits):
        packed = jnp.where(differing == (1 << b), b, packed)
    slot = jnp.where(
        slot < cells,
        slot,
        jnp.where(
            shifted < n_gy * ghosts,
            cells + packed * ghosts + within,
            slot - (n_gy - bits) * ghosts,
        ),
    )
    for f in range(6):
        for at in range(0, cells, LANES):
            part = jnp.broadcast_to(slot[f : f + 1, at : at + LANES], (rows, LANES))
            lane = jnp.bitwise_and(part, LANES - 1)
            block_id = jnp.right_shift(part, 7)
            for group in range(2 * fields):
                blocks = [
                    sources[i, group * rows : (group + 1) * rows, :]
                    for i in range(n_blocks)
                ]
                hi, lo = split(lane_gather(blocks, lane, block_id))
                if group < fields:
                    u_hi[group, f, :, at : at + LANES] = hi
                    u_lo[group, f, :, at : at + LANES] = lo
                else:
                    k = group - fields
                    z_hi[k, f * rows : (f + 1) * rows, at : at + LANES] = hi
                    z_lo[k, f * rows : (f + 1) * rows, at : at + LANES] = lo

    column = lax.broadcasted_iota(jnp.int32, (hang_rows, cells), 1).astype(F32)
    place_wide = jnp.broadcast_to(place_rows, (hang_rows, cells))
    scatter = [
        jnp.where(place_wide == column + float(f * cells), 1.0, 0.0).astype(BF16) for f in range(6)
    ]
    coef = coef_ref[...]
    size = jnp.exp2(-levels_ref[...].astype(F32))
    zero = jnp.zeros((rows, cells), BF16)
    child_masks = []
    for f in range(6):
        wide = jnp.broadcast_to(child_ref[f : f + 1, :], (rows, cells))
        child_masks.append([wide == h for h in range(children + 1)])

    face_wide = jnp.broadcast_to(lane_face, (rows, hang_pad))
    child_wide = jnp.broadcast_to(lane_child, (rows, hang_pad))
    fine_masks = [face_wide == (f ^ 1) for f in range(6)]
    place_masks = [child_wide == h for h in range(children)]
    hang_zero = jnp.zeros((rows, hang_pad), BF16)

    for k in range(fields):
        own_u, own_z = [
            jnp.concatenate(
                [sources[i, at * rows : (at + 1) * rows, :] for i in range(own_blocks)], 1
            )
            for at in (k, fields + k)
        ]
        own_z_hi, own_z_lo = split(own_z)
        weight = dot3(
            recon_both[:, 0 : 7 * rows],
            jnp.concatenate([own_z_hi, z_hi[k]], 0),
            jnp.concatenate([own_z_lo, z_lo[k]], 0),
        )
        src_hi, src_lo = split(
            jnp.concatenate(
                [source_flat[i, pl.ds(k, rows, stride=fields), :] for i in range(own_blocks)], 1
            )
        )
        scaled_hi, scaled_lo = split(-coef * own_u)
        residual = dot3(
            res_both[:, 0 : 2 * rows],
            jnp.concatenate([src_hi, scaled_hi], 0),
            jnp.concatenate([src_lo, scaled_lo], 0),
        )
        cell_part = jnp.sum(residual * weight, axis=0, keepdims=True)
        cell_ref[k : k + 1, :] = size * cell_part * (1.0 / math.sqrt(quads))
        w_hi, w_lo = split(weight)
        face_weight = dot3(face_both, w_hi, w_lo)

        hang_parts = split(hang_flat[pl.ds(k, rows, stride=fields), :])
        hang_hi, hang_lo = [
            jnp.concatenate([jnp.where(m, x, hang_zero) for m in fine_masks], 0) for x in hang_parts
        ]
        trace_parts = split(dot3(flux_both, hang_hi, hang_lo))
        trace_hi, trace_lo = [
            jnp.concatenate([jnp.where(m, x, hang_zero) for m in place_masks], 0)
            for x in trace_parts
        ]
        traces = dot3(back_both, trace_hi, trace_lo)
        trace_both = jnp.concatenate(split(traces), 0)[:, 0:hang_rows]

        own_u_hi, own_u_lo = split(own_u)
        product = jnp.zeros((rows, cells), F32)
        for f in range(6):
            near_hi = u_hi[k, f]
            near_lo = u_lo[k, f]
            masks = child_masks[f]
            hi = jnp.concatenate([jnp.where(m, near_hi, zero) for m in masks] + [own_u_hi], 0)
            lo = jnp.concatenate([jnp.where(m, near_lo, zero) for m in masks] + [own_u_lo], 0)
            jump = dot3(map_both[f], hi, lo)
            extra = mm(trace_both, scatter[f])
            jump = jump + extra[0:rows] + extra[rows:]
            product = product + jump * face_weight[f * rows : (f + 1) * rows]
        face_part = jnp.sum(product, axis=0, keepdims=True)
        face_ref[k : k + 1, :] = size * face_part * (1.0 / math.sqrt(6 * points))


def solution(mesh):
    n_gx, n_gy = mesh.shape["gx"], mesh.shape["gy"]
    bits = n_gy.bit_length() - 1
    vmem = pl.BlockSpec(memory_space=pltpu.VMEM)

    def shards(
        primal,
        adjoint,
        source,
        coefficient,
        levels,
        recon,
        stiffness,
        interp,
        flux,
        face_eval,
        child_interp,
        ghost_send,
        edge_send,
        neighbor_slot,
        neighbor_child,
        hang_send,
        hang_recv,
    ):
        fields, dofs, cells = primal.shape
        ghosts, edges, hangs = ghost_send.shape[2], edge_send.shape[2], hang_send.shape[3]
        rows = round_up(dofs, 32)
        quads = recon.shape[1]
        quad_rows = round_up(quads, LANES)
        dims = (n_gx, n_gy, bits, ghosts, edges, hangs, fields, rows)
        primal, adjoint, source = [x.transpose(1, 0, 2) for x in (primal, adjoint, source)]
        main_pad = round_up(bits * ghosts + 2 * edges, LANES)
        hang_pad = round_up(bits * hangs, LANES)
        wide = 2 * fields * rows
        from_gy, from_gx = pl.pallas_call(
            functools.partial(exchange_kernel, dims),
            out_shape=(
                jax.ShapeDtypeStruct((bits, ghosts + hangs, wide), F32),
                jax.ShapeDtypeStruct((2, edges, wide), F32),
            ),
            in_specs=[vmem] * 5,
            out_specs=(vmem, vmem),
            scratch_shapes=[
                pltpu.VMEM((bits, ghosts + hangs, wide), F32),
                pltpu.VMEM((2, edges, wide), F32),
                pltpu.VMEM((8, main_pad + hang_pad), jnp.int32),
                pltpu.VMEM((wide, LANES), F32),
                pltpu.VMEM((cells // LANES, wide, LANES), F32),
                pltpu.SemaphoreType.DMA((bits,)),
                pltpu.SemaphoreType.DMA((bits,)),
                pltpu.SemaphoreType.DMA((2,)),
                pltpu.SemaphoreType.DMA((2,)),
            ],
            compiler_params=pltpu.CompilerParams(collective_id=0, has_side_effects=True),
            name="exchange",
        )(primal, adjoint, ghost_send, edge_send, hang_send)
        out = jax.ShapeDtypeStruct((fields, cells), F32)
        return pl.pallas_call(
            functools.partial(compute_kernel, dims),
            out_shape=(out, out),
            in_specs=[vmem] * 16,
            out_specs=(vmem, vmem),
            scratch_shapes=[
                pltpu.VMEM((8 * rows, quad_rows), F32),
                pltpu.VMEM((LANES, quad_rows), F32),
                pltpu.VMEM((6 * rows, quad_rows), F32),
                pltpu.VMEM((4 * rows, LANES), F32),
                pltpu.VMEM((4 * rows, LANES), F32),
                pltpu.VMEM((rows, round_up(6 * rows, LANES)), F32),
                pltpu.VMEM((6, rows, 6 * rows), F32),
                pltpu.VMEM((8, hang_pad), jnp.int32),
                pltpu.VMEM((fields, 6 * rows, cells), BF16),
                pltpu.VMEM((fields, 6 * rows, cells), BF16),
                pltpu.VMEM((fields, 6, rows, cells), BF16),
                pltpu.VMEM((fields, 6, rows, cells), BF16),
                pltpu.VMEM(((cells + main_pad) // LANES, wide, LANES), F32),
                pltpu.VMEM(((cells + main_pad) // LANES, wide, LANES), F32),
                pltpu.VMEM((cells // LANES, fields * rows, LANES), F32),
                pltpu.VMEM((fields * rows, hang_pad), F32),
            ],
            name="indicators",
        )(
            primal,
            adjoint,
            source,
            coefficient.reshape(1, cells),
            levels.reshape(1, cells),
            recon.transpose(2, 0, 1),
            stiffness.T,
            interp.T,
            flux,
            face_eval,
            child_interp.transpose(1, 0, 2),
            neighbor_slot,
            neighbor_child,
            hang_recv,
            from_gy,
            from_gx,
        )

    both = ("gx", "gy")
    placed = (
        P(None, None, both),
        P(None, None, both),
        P(None, None, both),
        P(both),
        P(both),
        P(),
        P(),
        P(),
        P(),
        P(),
        P(),
        P(both, None, None),
        P(both, None, None),
        P(None, both),
        P(None, both),
        P(None, both, None, None),
        P(None, both, None, None),
    )
    return jax.shard_map(
        shards,
        mesh=mesh,
        in_specs=placed,
        out_specs=(P(None, both), P(None, both)),
        check_vma=False,
    )
```

```python
import functools
import math

import jax
import jax.numpy as jnp
from jax import lax
from jax.experimental import pallas as pl
from jax.experimental.pallas import tpu as pltpu
from jax.sharding import PartitionSpec as P

LANES = 128
F32 = jnp.float32
BF16 = jnp.bfloat16
MESH = pl.DeviceIdType.MESH


def round_up(value, unit):
    return -(-value // unit) * unit


def split(x):
    hi = x.astype(BF16)
    lo = (x - hi.astype(F32)).astype(BF16)
    return hi, lo


def mm(a, b):
    return jnp.dot(a, b, preferred_element_type=F32)


def dot3(a_both, b_hi, b_lo):
    rows = a_both.shape[0] // 2
    first = mm(a_both, b_hi)
    return first[:rows] + first[rows:] + mm(a_both[:rows], b_lo)


def fill_flat(flat, refs, width):
    for at, ref in enumerate(refs):
        dofs, fields, cells = ref.shape
        used = dofs * fields
        for i in range(cells // LANES):
            for j in range(dofs):
                row = at * width + j * fields
                flat[i, row : row + fields, :] = ref[j, :, i * LANES : (i + 1) * LANES]
            flat[i, at * width + used : (at + 1) * width, :] = jnp.zeros((width - used, LANES), F32)


def lane_gather(blocks, lane, block_id):
    total = jnp.zeros(blocks[0].shape, F32)
    for i, block in enumerate(blocks):
        got = jnp.take_along_axis(block, lane, axis=1)
        total = jnp.where(block_id == i, got, total)
    return total


def compute_kernel(
    dims,
    primal_ref,
    adjoint_ref,
    source_ref,
    coef_ref,
    levels_ref,
    recon_ref,
    stiffness_ref,
    interp_ref,
    flux_ref,
    face_eval_ref,
    child_interp_ref,
    slot_ref,
    child_ref,
    hang_ref,
    ghost_ref,
    edge_ref,
    hang_send_ref,
    cell_ref,
    face_ref,
    op_recon,
    op_res,
    op_face,
    op_child,
    child_flat,
    op_flux,
    op_map,
    maps,
    z_hi,
    z_lo,
    u_hi,
    u_lo,
    sources,
    flat,
    source_flat,
    hang_flat,
    near,
    residuals,
    from_gy,
    from_gx,
    to_gy,
    to_gx,
    ids,
    packed,
    send_gy,
    recv_gy,
    send_gx,
    recv_gx,
):
    n_gx, n_gy, bits, ghosts, edges, hangs, fields, rows = dims
    gx = lax.axis_index("gx")
    gy = lax.axis_index("gy")
    dofs, _, cells = primal_ref.shape
    width = fields * rows
    partners = [jnp.bitwise_xor(gy, 1 << b) for b in range(bits)]

    barrier = pltpu.get_barrier_semaphore()
    for partner in partners:
        pl.semaphore_signal(barrier, inc=1, device_id=(gx, partner), device_id_type=MESH)

    @pl.when(gx > 0)
    def _():
        pl.semaphore_signal(barrier, inc=1, device_id=(gx - 1, gy), device_id_type=MESH)

    @pl.when(gx < n_gx - 1)
    def _():
        pl.semaphore_signal(barrier, inc=1, device_id=(gx + 1, gy), device_id_type=MESH)

    main = bits * ghosts + 2 * edges
    main_pad = round_up(main, LANES)
    hang_pad = round_up(bits * hangs, LANES)
    ids[...] = jnp.zeros_like(ids)
    for b, partner in enumerate(partners):
        ids[0:1, b * ghosts : (b + 1) * ghosts] = ghost_ref[0, pl.ds(partner, 1), :]
        at = main_pad + b * hangs
        ids[0:1, at : at + hangs] = hang_send_ref[0, 0, pl.ds(partner, 1), :]
    for side in range(2):
        at = bits * ghosts + side * edges
        ids[0:1, at : at + edges] = edge_ref[0, side : side + 1, :]
    fill_flat(flat, (primal_ref, adjoint_ref), width)
    chosen = jnp.maximum(ids[0:1, :], 0)
    for at in range(0, main_pad + hang_pad, LANES):
        part = jnp.broadcast_to(chosen[:, at : at + LANES], (rows, LANES))
        lane = jnp.bitwise_and(part, LANES - 1)
        block_id = jnp.right_shift(part, 7)
        count = 2 * fields if at < main_pad else fields
        for group in range(count):
            blocks = [flat[i, group * rows : (group + 1) * rows, :] for i in range(cells // LANES)]
            packed[group * rows : (group + 1) * rows, :] = lane_gather(blocks, lane, block_id)
        if at < main_pad:
            turned = packed[...].T
            for first in range(at, min(at + LANES, main), edges):
                chunk = turned[first - at : first - at + edges]
                if first < bits * ghosts:
                    inner = first % ghosts
                    to_gy[first // ghosts, inner : inner + edges, :] = chunk
                else:
                    to_gx[(first - bits * ghosts) // edges] = chunk
        else:
            turned = packed[0:width, :].T
            for b in range(bits):
                at_slot = b * hangs - (at - main_pad)
                if 0 <= at_slot < LANES:
                    to_gy[b, ghosts : ghosts + hangs, 0:width] = turned[at_slot : at_slot + hangs]
                    to_gy[b, ghosts : ghosts + hangs, width:] = jnp.zeros(
                        (hangs, to_gy.shape[2] - width), F32
                    )

    def low_copy():
        return pltpu.make_async_remote_copy(
            src_ref=to_gx.at[0],
            dst_ref=from_gx.at[1],
            send_sem=send_gx.at[0],
            recv_sem=recv_gx.at[1],
            device_id=(gx - 1, gy),
            device_id_type=MESH,
        )

    def high_copy():
        return pltpu.make_async_remote_copy(
            src_ref=to_gx.at[1],
            dst_ref=from_gx.at[0],
            send_sem=send_gx.at[1],
            recv_sem=recv_gx.at[0],
            device_id=(gx + 1, gy),
            device_id_type=MESH,
        )

    @pl.when((gx > 0) & (gx < n_gx - 1))
    def _():
        pl.semaphore_wait(barrier, bits + 2)

    @pl.when((gx == 0) | (gx == n_gx - 1))
    def _():
        pl.semaphore_wait(barrier, bits + (1 if n_gx > 1 else 0))

    copies = []
    for b in reversed(range(bits)):
        copy = pltpu.make_async_remote_copy(
            src_ref=to_gy.at[b],
            dst_ref=from_gy.at[b],
            send_sem=send_gy.at[b],
            recv_sem=recv_gy.at[b],
            device_id=(gx, partners[b]),
            device_id_type=MESH,
        )
        copy.start()
        copies.append(copy)

    @pl.when(gx > 0)
    def _():
        low_copy().start()

    @pl.when(gx == 0)
    def _():
        from_gx[0] = jnp.zeros(from_gx.shape[1:], F32)

    @pl.when(gx < n_gx - 1)
    def _():
        high_copy().start()

    @pl.when(gx == n_gx - 1)
    def _():
        from_gx[1] = jnp.zeros(from_gx.shape[1:], F32)

    quads = recon_ref.shape[2]
    own_blocks = cells // LANES
    points = flux_ref.shape[1]
    remote = bits * ghosts + 2 * edges
    remote_pad = round_up(remote, LANES)
    hang_count = bits * hangs
    hang_pad = round_up(hang_count, LANES)
    hang_rows = round_up(hang_count, 16)
    children = 4

    op_recon[...] = jnp.zeros_like(op_recon)
    op_res[...] = jnp.zeros_like(op_res)
    op_face[...] = jnp.zeros_like(op_face)
    child_flat[...] = jnp.zeros_like(child_flat)
    op_flux[...] = jnp.zeros_like(op_flux)
    for j in range(dofs):
        op_recon[8 * j : 8 * j + 7, 0:quads] = recon_ref[j]
    op_res[0:dofs, 0:quads] = interp_ref[...]
    op_res[rows : rows + dofs, 0:quads] = stiffness_ref[...]
    for f in range(6):
        op_face[f * rows : f * rows + points, 0:quads] = face_eval_ref[f]
        op_flux[0:points, f * rows : f * rows + dofs] = flux_ref[f]
    for p in range(points):
        child_flat[children * p : children * (p + 1), 0:points] = child_interp_ref[p]
    for h in range(children):
        op_child[h * rows : (h + 1) * rows, :] = child_flat[pl.ds(h, rows, stride=children), :]
    flux_all = op_flux[...]
    flux_hi, flux_lo = split(flux_all)
    child_both = jnp.concatenate(split(op_child[...]), 0)
    mapped_ops = dot3(child_both[:, 0:rows], flux_hi, flux_lo)
    for f in range(6):
        opp = f ^ 1
        for h in range(children):
            op_map[f, :, h * rows : (h + 1) * rows] = mapped_ops[
                h * rows : (h + 1) * rows, opp * rows : (opp + 1) * rows
            ]
        op_map[f, :, 4 * rows : 5 * rows] = flux_all[:, opp * rows : (opp + 1) * rows]
        op_map[f, :, 5 * rows : 6 * rows] = flux_all[:, f * rows : (f + 1) * rows]
    recon_turned = [op_recon[pl.ds(f, rows, stride=8), :] for f in range(8)]
    recon_both = jnp.concatenate(split(jnp.concatenate(recon_turned, 0).T), 0)
    res_both = jnp.concatenate(split(op_res[...].T), 0)
    face_both = jnp.concatenate(split(op_face[...]), 0)
    flux_both = jnp.concatenate([flux_hi, flux_lo], 0)[:, 0 : 6 * rows]
    back_both = jnp.concatenate(split(op_child[...].T[0:rows]), 0)
    map_both = [jnp.concatenate(split(op_map[f]), 0) for f in range(6)]

    maps[...] = jnp.full(maps.shape, -1, jnp.int32)
    for b in range(bits):
        partner = jnp.bitwise_xor(gy, 1 << b)
        for i in range(3):
            maps[i : i + 1, b * hangs : (b + 1) * hangs] = hang_ref[i, 0, pl.ds(partner, 1), :]
    lane_face = maps[1:2, :]
    lane_child = maps[2:3, :]
    live = maps[0:1, :] >= 0
    place = jnp.where(live, maps[0:1, :] + lane_face * cells, -1).astype(F32)
    place_rows = jnp.broadcast_to(place, (LANES, hang_pad)).T[0:hang_rows, 0:1]

    fill_flat(source_flat, (source_ref,), width)
    for i in range(own_blocks):
        for group in range(2 * fields):
            first = group // fields * width + group % fields
            sources[i, group * rows : (group + 1) * rows, :] = flat[
                i, pl.ds(first, rows, stride=fields), :
            ]

    slot = slot_ref[...]
    shifted = slot - cells
    log_ghosts = ghosts.bit_length() - 1
    peer = jnp.right_shift(shifted, log_ghosts)
    within = jnp.bitwise_and(shifted, ghosts - 1)
    differing = jnp.bitwise_xor(peer, gy)
    place_of = jnp.zeros_like(slot)
    for b in range(1, bits):
        place_of = jnp.where(differing == (1 << b), b, place_of)
    slot = jnp.where(
        slot < cells,
        slot,
        jnp.where(
            shifted < n_gy * ghosts,
            cells + place_of * ghosts + within,
            slot - (n_gy - bits) * ghosts,
        ),
    )
    coef = coef_ref[...]
    for k in range(fields):
        own_u = jnp.concatenate(
            [sources[i, k * rows : (k + 1) * rows, :] for i in range(own_blocks)], 1
        )
        src_hi, src_lo = split(
            jnp.concatenate(
                [source_flat[i, pl.ds(k, rows, stride=fields), :] for i in range(own_blocks)], 1
            )
        )
        scaled_hi, scaled_lo = split(-coef * own_u)
        residuals[k] = dot3(
            res_both[:, 0 : 2 * rows],
            jnp.concatenate([src_hi, scaled_hi], 0),
            jnp.concatenate([src_lo, scaled_lo], 0),
        )

    for f in range(6):
        for at in range(0, cells, LANES):
            part = jnp.broadcast_to(slot[f : f + 1, at : at + LANES], (rows, LANES))
            lane = jnp.bitwise_and(part, LANES - 1)
            block_id = jnp.right_shift(part, 7)
            for group in range(2 * fields):
                span = slice(group * rows, (group + 1) * rows)
                blocks = [sources[i, span, :] for i in range(own_blocks)]
                near[f, at // LANES, span, :] = lane_gather(blocks, lane, block_id)

    for copy in copies:
        copy.wait()

    @pl.when(gx > 0)
    def _():
        low_copy().wait_send()
        high_copy().wait_recv()

    @pl.when(gx < n_gx - 1)
    def _():
        high_copy().wait_send()
        low_copy().wait_recv()

    parts = [from_gy[b, 0:ghosts, :] for b in range(bits)] + [from_gx[0], from_gx[1]]
    if remote_pad > remote:
        parts.append(jnp.zeros((remote_pad - remote, parts[0].shape[1]), F32))
    arrived = jnp.concatenate(parts, 0).T
    for i in range(remote_pad // LANES):
        flat[own_blocks + i] = arrived[:, i * LANES : (i + 1) * LANES]
    n_blocks = own_blocks + remote_pad // LANES
    for i in range(own_blocks, n_blocks):
        for group in range(2 * fields):
            first = group // fields * width + group % fields
            sources[i, group * rows : (group + 1) * rows, :] = flat[
                i, pl.ds(first, rows, stride=fields), :
            ]
    parts = [from_gy[b, ghosts : ghosts + hangs, 0:width] for b in range(bits)]
    parts.append(jnp.zeros((hang_pad - hang_count, width), F32))
    hang_flat[...] = jnp.concatenate(parts, 0).T

    for f in range(6):
        for at in range(0, cells, LANES):
            part = jnp.broadcast_to(slot[f : f + 1, at : at + LANES], (rows, LANES))
            lane = jnp.bitwise_and(part, LANES - 1)
            block_id = jnp.right_shift(part, 7)
            for group in range(2 * fields):
                span = slice(group * rows, (group + 1) * rows)
                total = near[f, at // LANES, span, :]
                for i in range(own_blocks, n_blocks):
                    got = jnp.take_along_axis(sources[i, span, :], lane, axis=1)
                    total = jnp.where(block_id == i, got, total)
                hi, lo = split(total)
                if group < fields:
                    u_hi[group, f, :, at : at + LANES] = hi
                    u_lo[group, f, :, at : at + LANES] = lo
                else:
                    k = group - fields
                    z_hi[k, f * rows : (f + 1) * rows, at : at + LANES] = hi
                    z_lo[k, f * rows : (f + 1) * rows, at : at + LANES] = lo

    column = lax.broadcasted_iota(jnp.int32, (hang_rows, cells), 1).astype(F32)
    place_wide = jnp.broadcast_to(place_rows, (hang_rows, cells))
    scatter = [
        jnp.where(place_wide == column + float(f * cells), 1.0, 0.0).astype(BF16) for f in range(6)
    ]
    size = jnp.exp2(-levels_ref[...].astype(F32))
    zero = jnp.zeros((rows, cells), BF16)
    child_masks = []
    for f in range(6):
        wide = jnp.broadcast_to(child_ref[f : f + 1, :], (rows, cells))
        child_masks.append([wide == h for h in range(children + 1)])

    face_wide = jnp.broadcast_to(lane_face, (rows, hang_pad))
    child_wide = jnp.broadcast_to(lane_child, (rows, hang_pad))
    fine_masks = [face_wide == (f ^ 1) for f in range(6)]
    place_masks = [child_wide == h for h in range(children)]
    hang_zero = jnp.zeros((rows, hang_pad), BF16)

    for k in range(fields):
        own_u, own_z = [
            jnp.concatenate(
                [sources[i, at * rows : (at + 1) * rows, :] for i in range(own_blocks)], 1
            )
            for at in (k, fields + k)
        ]
        own_z_hi, own_z_lo = split(own_z)
        weight = dot3(
            recon_both[:, 0 : 7 * rows],
            jnp.concatenate([own_z_hi, z_hi[k]], 0),
            jnp.concatenate([own_z_lo, z_lo[k]], 0),
        )
        residual = residuals[k]
        cell_part = jnp.sum(residual * weight, axis=0, keepdims=True)
        cell_ref[k : k + 1, :] = size * cell_part * (1.0 / math.sqrt(quads))
        w_hi, w_lo = split(weight)
        face_weight = dot3(face_both, w_hi, w_lo)

        hang_parts = split(hang_flat[pl.ds(k, rows, stride=fields), :])
        hang_hi, hang_lo = [
            jnp.concatenate([jnp.where(m, x, hang_zero) for m in fine_masks], 0) for x in hang_parts
        ]
        trace_parts = split(dot3(flux_both, hang_hi, hang_lo))
        trace_hi, trace_lo = [
            jnp.concatenate([jnp.where(m, x, hang_zero) for m in place_masks], 0)
            for x in trace_parts
        ]
        traces = dot3(back_both, trace_hi, trace_lo)
        trace_both = jnp.concatenate(split(traces), 0)[:, 0:hang_rows]

        own_u_hi, own_u_lo = split(own_u)
        product = jnp.zeros((rows, cells), F32)
        for f in range(6):
            near_hi = u_hi[k, f]
            near_lo = u_lo[k, f]
            masks = child_masks[f]
            hi = jnp.concatenate([jnp.where(m, near_hi, zero) for m in masks] + [own_u_hi], 0)
            lo = jnp.concatenate([jnp.where(m, near_lo, zero) for m in masks] + [own_u_lo], 0)
            jump = dot3(map_both[f], hi, lo)
            extra = mm(trace_both, scatter[f])
            jump = jump + extra[0:rows] + extra[rows:]
            product = product + jump * face_weight[f * rows : (f + 1) * rows]
        face_part = jnp.sum(product, axis=0, keepdims=True)
        face_ref[k : k + 1, :] = size * face_part * (1.0 / math.sqrt(6 * points))


def solution(mesh):
    n_gx, n_gy = mesh.shape["gx"], mesh.shape["gy"]
    bits = n_gy.bit_length() - 1
    vmem = pl.BlockSpec(memory_space=pltpu.VMEM)

    def shards(
        primal,
        adjoint,
        source,
        coefficient,
        levels,
        recon,
        stiffness,
        interp,
        flux,
        face_eval,
        child_interp,
        ghost_send,
        edge_send,
        neighbor_slot,
        neighbor_child,
        hang_send,
        hang_recv,
    ):
        fields, dofs, cells = primal.shape
        ghosts, edges, hangs = ghost_send.shape[2], edge_send.shape[2], hang_send.shape[3]
        rows = round_up(dofs, 32)
        quads = recon.shape[1]
        quad_rows = round_up(quads, LANES)
        dims = (n_gx, n_gy, bits, ghosts, edges, hangs, fields, rows)
        primal, adjoint, source = [x.transpose(1, 0, 2) for x in (primal, adjoint, source)]
        main_pad = round_up(bits * ghosts + 2 * edges, LANES)
        hang_pad = round_up(bits * hangs, LANES)
        wide = 2 * fields * rows
        out = jax.ShapeDtypeStruct((fields, cells), F32)
        return pl.pallas_call(
            functools.partial(compute_kernel, dims),
            out_shape=(out, out),
            in_specs=[vmem] * 17,
            out_specs=(vmem, vmem),
            scratch_shapes=[
                pltpu.VMEM((8 * rows, quad_rows), F32),
                pltpu.VMEM((LANES, quad_rows), F32),
                pltpu.VMEM((6 * rows, quad_rows), F32),
                pltpu.VMEM((4 * rows, LANES), F32),
                pltpu.VMEM((4 * rows, LANES), F32),
                pltpu.VMEM((rows, round_up(6 * rows, LANES)), F32),
                pltpu.VMEM((6, rows, 6 * rows), F32),
                pltpu.VMEM((8, hang_pad), jnp.int32),
                pltpu.VMEM((fields, 6 * rows, cells), BF16),
                pltpu.VMEM((fields, 6 * rows, cells), BF16),
                pltpu.VMEM((fields, 6, rows, cells), BF16),
                pltpu.VMEM((fields, 6, rows, cells), BF16),
                pltpu.VMEM(((cells + main_pad) // LANES, wide, LANES), F32),
                pltpu.VMEM(((cells + main_pad) // LANES, wide, LANES), F32),
                pltpu.VMEM((cells // LANES, fields * rows, LANES), F32),
                pltpu.VMEM((fields * rows, hang_pad), F32),
                pltpu.VMEM((6, cells // LANES, wide, LANES), F32),
                pltpu.VMEM((fields, quad_rows, cells), F32),
                pltpu.VMEM((bits, ghosts + hangs, wide), F32),
                pltpu.VMEM((2, edges, wide), F32),
                pltpu.VMEM((bits, ghosts + hangs, wide), F32),
                pltpu.VMEM((2, edges, wide), F32),
                pltpu.VMEM((8, main_pad + hang_pad), jnp.int32),
                pltpu.VMEM((wide, LANES), F32),
                pltpu.SemaphoreType.DMA((bits,)),
                pltpu.SemaphoreType.DMA((bits,)),
                pltpu.SemaphoreType.DMA((2,)),
                pltpu.SemaphoreType.DMA((2,)),
            ],
            compiler_params=pltpu.CompilerParams(collective_id=0, has_side_effects=True),
            name="indicators",
        )(
            primal,
            adjoint,
            source,
            coefficient.reshape(1, cells),
            levels.reshape(1, cells),
            recon.transpose(2, 0, 1),
            stiffness.T,
            interp.T,
            flux,
            face_eval,
            child_interp.transpose(1, 0, 2),
            neighbor_slot,
            neighbor_child,
            hang_recv,
            ghost_send,
            edge_send,
            hang_send,
        )

    both = ("gx", "gy")
    placed = (
        P(None, None, both),
        P(None, None, both),
        P(None, None, both),
        P(both),
        P(both),
        P(),
        P(),
        P(),
        P(),
        P(),
        P(),
        P(both, None, None),
        P(both, None, None),
        P(None, both),
        P(None, both),
        P(None, both, None, None),
        P(None, both, None, None),
    )
    return jax.shard_map(
        shards,
        mesh=mesh,
        in_specs=placed,
        out_specs=(P(None, both), P(None, both)),
        check_vma=False,
    )
```
